32 devices in a mesh: slab: 2 (over y), date: 8 (over z, x), tile: 1, sub: 2 (over core).
Axes of the slice: x: 2, y: 2, z: 4, core: 2. Of those that a mesh axis runs over, the one named last changes fastest.
Arguments:
- slc: bfloat16 [2, 100, 128, 512], P(None, None, 'date', ('slab', 'tile', 'sub')), parts along dimension 3, may hold values from -300 to 300, as said below
- usable: int32 [100, 128, 512], P(None, 'date', ('slab', 'tile', 'sub')), parts along dimension 2, may hold values 0 or 1
Outputs:
- coherence: bfloat16 [2, 4, 8, 16, 128, 128], P(None, ('slab', 'tile', 'sub'), 'date'), parts along dimension 1
- linked: float32 [2, 128, 512], P(None, 'date', ('slab', 'tile', 'sub')), parts along dimension 2
The draws below stay inside these ranges and needn't reach their ends.
There are 2 independent parts, one for each index of `slab`. The reference program is written for one: setup_inputs(seed, part) draws one part's arguments, and reference() takes and returns one part's arrays. A program takes and returns all parts, laid end to end along the dimension named above; each array names one. Nothing has to cross between parts.
Inputs may be any that keep to these rules, and one draw needn't show every extreme that they name: `slc`: complex samples of a partly coherent stack.
All inputs are finite; a program needn't handle non-finite values. No bound on the sum of `usable` on one device may be relied on, other than what follows from the above.
Results may differ from the reference program's by a relative error of at most 0.0016.
Values may be sent and summed in bfloat16 or wider, within the bound.
A program may use at most 64 MiB of HBM per device.

```python
import math
import jax
import jax.numpy as jnp
from jax import lax

DATES = 128
LOOKS = 100
ITERS = 4
WD = 16
WT = 128
NG = 2
NB = 8
WIN = 256


def rotate(common, phase):
    cosine = jnp.cos(phase)[None]
    sine_part = jnp.sin(phase)[None]
    return jnp.stack([common[0] * cosine - common[1] * sine_part, common[0] * sine_part + common[1] * cosine])


def draw_slc(key, part):
    subkeys = jax.random.split(key, 9)
    grid_shape = (DATES, WIN)
    amplitude = jnp.exp(jax.random.uniform(subkeys[0], grid_shape, jnp.float32, 0.0, math.log(10.0)))
    speckle = jnp.clip(jax.random.normal(subkeys[8], (2, LOOKS, DATES, WIN), jnp.float32), -4.0, 4.0)
    first_phase = jax.random.uniform(subkeys[1], grid_shape, jnp.float32, -math.pi, math.pi)
    second_phase = jax.random.uniform(subkeys[2], grid_shape, jnp.float32, -math.pi, math.pi)
    first_weight = jax.random.uniform(subkeys[3], (WIN,), jnp.float32, 0.3, 0.9)
    second_weight = jax.random.uniform(subkeys[4], (WIN,), jnp.float32, 0.1, 0.4)
    first_common = jnp.clip(jax.random.normal(subkeys[5], (2, LOOKS, 1, WIN), jnp.float32), -4.0, 4.0)
    second_common = jnp.clip(jax.random.normal(subkeys[6], (2, LOOKS, 1, WIN), jnp.float32), -4.0, 4.0)
    noise_weight = jnp.sqrt(jnp.maximum(1.0 - first_weight * first_weight - second_weight * second_weight, 0.05))
    sample = first_weight * rotate(first_common, first_phase) + second_weight * rotate(second_common, second_phase) + noise_weight * speckle
    return (amplitude * sample).astype(jnp.bfloat16)


def set_ends(drawn, stream_key, low, high):
    dims = drawn.shape
    place = [jax.random.randint(jax.random.fold_in(stream_key, axis), (), 0, dims[axis]) for axis in range(len(dims))]
    drawn = drawn.at[tuple(place)].set(low)
    longest = dims.index(max(dims))
    place[longest] = (place[longest] + 1) % dims[longest]
    return drawn.at[tuple(place)].set(high)


def setup_inputs(seed: int = 0, part: int = 0) -> dict:
    seeds = jax.random.split(jax.random.key(seed), 3)
    own_keys = jax.random.split(jax.random.fold_in(seeds[2], part), 3)
    return {
        "slc": draw_slc(jax.random.fold_in(jax.random.fold_in(seeds[2], part), 71), part),
        "usable": set_ends((jax.random.randint(own_keys[1], (LOOKS, DATES, WIN), 0, 4) < 3).astype(jnp.int32), jax.random.fold_in(own_keys[1], 1), 0, 1),
    }


def link_vectors(coherence):
    matrix = coherence.astype(jnp.float32)
    vec_real = jnp.ones((DATES, matrix.shape[1]), jnp.float32)
    vec_imag = jnp.zeros((DATES, matrix.shape[1]), jnp.float32)
    for step in range(ITERS):
        rr = jnp.einsum('wab,bw->aw', matrix[0], vec_real, precision=lax.Precision.HIGHEST)
        ii = jnp.einsum('wab,bw->aw', matrix[1], vec_imag, precision=lax.Precision.HIGHEST)
        ri = jnp.einsum('wab,bw->aw', matrix[0], vec_imag, precision=lax.Precision.HIGHEST)
        ir = jnp.einsum('wab,bw->aw', matrix[1], vec_real, precision=lax.Precision.HIGHEST)
        new_real = rr - ii
        new_imag = ri + ir
        scale = lax.rsqrt(lax.optimization_barrier(jnp.mean(new_real * new_real + new_imag * new_imag, axis=0)) + 1e-05)
        vec_real = new_real * scale[None]
        vec_imag = new_imag * scale[None]
    return jnp.stack([vec_real, vec_imag])

def window_block(operands):
    block, root = operands
    real_sum = jnp.einsum('law,lbw->wab', block[0], block[0]) + jnp.einsum('law,lbw->wab', block[1], block[1])
    imag_sum = jnp.einsum('law,lbw->wab', block[1], block[0]) - jnp.einsum('law,lbw->wab', block[0], block[1])
    factor = root.T[:, :, None] * root.T[:, None, :] * (1.0 / LOOKS)
    coherence = jnp.stack([real_sum * factor, imag_sum * factor]).astype(jnp.bfloat16)
    return (coherence, link_vectors(coherence))

def reference(slc, usable):
    masked = slc * usable.astype(jnp.bfloat16)[None]
    samples = masked.astype(jnp.float32)
    intensity = lax.optimization_barrier(jnp.mean(samples[0] * samples[0] + samples[1] * samples[1], axis=0)) + 1e-05
    inverse_root = lax.rsqrt(intensity)
    blocks = jnp.moveaxis(samples.reshape(2, LOOKS, DATES, NG, WT), 3, 0)
    roots = jnp.moveaxis(inverse_root.reshape(DATES, NG, WT), 1, 0)
    coherence, linked = lax.map(window_block, (blocks, roots))
    coherence = jnp.moveaxis(coherence, 1, 0)
    linked = jnp.moveaxis(linked, 0, 2).reshape(2, DATES, WIN)
    return (coherence.reshape(2, NG, NB, WD, DATES, DATES), linked)
```

```python
import functools

import jax
import jax.numpy as jnp
from jax import lax
from jax.experimental import pallas as pl
from jax.experimental.pallas import tpu as pltpu
from jax.sharding import PartitionSpec as P

ITERS = 4
LANES = 128
NT = (((1,), (1,)), ((), ()))


def dot_nt(left, right):
    return lax.dot_general(left, right, NT, preferred_element_type=jnp.float32)


def window_coherence(real, imag, looks_count):
    dates = real.shape[0]
    plain = jnp.concatenate([real, imag], axis=1)
    swapped = jnp.concatenate([imag, -real], axis=1)
    sums = dot_nt(jnp.concatenate([plain, swapped], axis=0), plain)
    real_sum, imag_sum = sums[:dates], sums[dates:]
    rows = lax.broadcasted_iota(jnp.int32, (dates, dates), 0)
    columns = lax.broadcasted_iota(jnp.int32, (dates, dates), 1)
    diagonal = jnp.where(rows == columns, real_sum, 0.0)
    row_root = lax.rsqrt(jnp.sum(diagonal, axis=0, keepdims=True) * (1.0 / looks_count) + 1e-05)
    column_root = lax.rsqrt(jnp.sum(diagonal, axis=1, keepdims=True) * (1.0 / looks_count) + 1e-05)
    factor = column_root * row_root * (1.0 / looks_count)
    return (real_sum * factor).astype(jnp.bfloat16), (imag_sum * factor).astype(jnp.bfloat16)


def link_windows(matrices):
    dates = matrices[0].shape[1]
    row = lax.broadcasted_iota(jnp.int32, (8, dates), 0)
    is_real = row < 3
    is_imag = jnp.logical_and(row >= 3, row < 6)
    is_first = jnp.logical_or(row == 0, row == 3)
    is_second = jnp.logical_or(row == 1, row == 4)
    state = [jnp.where(is_real, 1.0, 0.0)] * len(matrices)
    result = None
    for step in range(ITERS):
        products = []
        for vec, matrix in zip(state, matrices):
            high = vec.astype(jnp.bfloat16).astype(jnp.float32)
            rest = vec - high
            middle = rest.astype(jnp.bfloat16).astype(jnp.float32)
            parts = jnp.where(is_first, high, jnp.where(is_second, middle, rest - middle))
            products.append(dot_nt(parts.astype(jnp.bfloat16), matrix))
        state, result = [], []
        for product in products:
            first, second = product[:, :dates], product[:, dates:]
            zero = jnp.zeros_like(first)
            new_real = jnp.sum(
                jnp.where(is_real, first, jnp.where(is_imag, -second, zero)), axis=0, keepdims=True
            )
            new_imag = jnp.sum(
                jnp.where(is_real, second, jnp.where(is_imag, first, zero)), axis=0, keepdims=True
            )
            power = jnp.sum(new_real * new_real + new_imag * new_imag, axis=1, keepdims=True)
            scale = lax.rsqrt(power * (1.0 / dates) + 1e-05)
            new_real = new_real * scale
            new_imag = new_imag * scale
            result.append((new_real, new_imag))
            state.append(
                jnp.where(
                    is_real,
                    jnp.broadcast_to(new_real, (8, dates)),
                    jnp.where(is_imag, jnp.broadcast_to(new_imag, (8, dates)), 0.0),
                )
            )
    return result


def kernel(
    count, looks_count, group,
    send_ref, coherence_ref, linked_ref,
    held, matrix, vectors, turned, landed,
    send_sem, recv_sem, own_sem, out_sem, back_send, back_recv,
):
    me = lax.axis_index("date")
    windows = held.shape[0]
    dates = held.shape[2]
    own = dates // count
    groups = windows // group

    barrier = pltpu.get_barrier_semaphore()
    for offset in range(1, count):
        pl.semaphore_signal(
            barrier, inc=1, device_id={"date": lax.rem(me + offset, count)},
            device_id_type=pl.DeviceIdType.MESH,
        )
    pl.semaphore_wait(barrier, count - 1)

    mine = pl.ds(pl.multiple_of(me * own, own), own)

    def block_copy(part, offset):
        span = pl.ds(part * group, group)
        other = lax.rem(me + offset, count)
        return pltpu.make_async_remote_copy(
            src_ref=send_ref.at[other, span],
            dst_ref=held.at[span, :, mine],
            send_sem=send_sem.at[part, offset],
            recv_sem=recv_sem.at[part, offset],
            device_id={"date": other},
            device_id_type=pl.DeviceIdType.MESH,
        )

    own_copy = pltpu.make_async_copy(send_ref.at[me], held.at[:, :, mine], own_sem)
    own_copy.start()

    def start_part(part, carry):
        for offset in range(1, count):
            block_copy(part, offset).start()
        return carry

    lax.fori_loop(0, groups, start_part, 0)
    own_copy.wait()

    def out_copy(part):
        span = pl.ds(part * group, group)
        return pltpu.make_async_copy(
            matrix.at[:, span], coherence_ref.at[:, 0, 0, span], out_sem.at[part]
        )

    def compute_part(part, carry):
        for offset in range(1, count):
            block_copy(part, offset).wait_recv()
        matrices = []
        for inner in range(group):
            window = part * group + inner
            real, imag = window_coherence(held[window, 0], held[window, 1], looks_count)
            matrix[0, window] = real
            matrix[1, window] = imag
            matrices.append(jnp.concatenate([real, imag], axis=0))
        for inner, (real, imag) in enumerate(link_windows(matrices)):
            vectors[0, pl.ds(part * group + inner, 1)] = real
            vectors[1, pl.ds(part * group + inner, 1)] = imag
        out_copy(part).start()
        return carry

    lax.fori_loop(0, groups, compute_part, 0)

    turned[:, : 2 * windows] = jnp.concatenate([vectors[0], vectors[1]], axis=0).T

    def back_copy(offset):
        other = lax.rem(me + offset, count)
        return pltpu.make_async_remote_copy(
            src_ref=turned.at[pl.ds(pl.multiple_of(other * own, own), own)],
            dst_ref=landed.at[me],
            send_sem=back_send.at[offset],
            recv_sem=back_recv.at[offset],
            device_id={"date": other},
            device_id_type=pl.DeviceIdType.MESH,
        )

    for offset in range(1, count):
        back_copy(offset).start()
    landed[me] = turned[mine]
    for offset in range(1, count):
        back_copy(offset).wait_recv()
    for side in range(2):
        linked_ref[side] = jnp.concatenate(
            [landed[source][:, side * windows : (side + 1) * windows] for source in range(count)], axis=1
        )

    def finish_part(part, carry):
        for offset in range(1, count):
            block_copy(part, offset).wait_send()
        out_copy(part).wait()
        return carry

    lax.fori_loop(0, groups, finish_part, 0)
    for offset in range(1, count):
        back_copy(offset).wait_send()


def local(slc, usable):
    looks_count, own_dates, windows = usable.shape
    count = lax.axis_size("date")
    per_device = windows // count
    dates = own_dates * count
    masked = slc * usable.astype(jnp.bfloat16)[None]
    padded_looks = pl.cdiv(looks_count, LANES) * LANES
    blocks = jnp.transpose(
        masked.reshape(2, looks_count, own_dates, count, per_device), (3, 4, 0, 2, 1)
    )
    blocks = jnp.pad(blocks, ((0, 0),) * 4 + ((0, padded_looks - looks_count),))
    group = next(size for size in (4, 2, 1) if per_device % size == 0)
    groups = per_device // group
    return pl.pallas_call(
        functools.partial(kernel, count, looks_count, group),
        out_shape=(
            jax.ShapeDtypeStruct((2, 1, 1, per_device, dates, dates), jnp.bfloat16),
            jax.ShapeDtypeStruct((2, own_dates, windows), jnp.float32),
        ),
        in_specs=[pl.BlockSpec(memory_space=pltpu.VMEM)],
        out_specs=(
            pl.BlockSpec(memory_space=pl.ANY),
            pl.BlockSpec(memory_space=pltpu.VMEM),
        ),
        scratch_shapes=[
            pltpu.VMEM((per_device, 2, dates, padded_looks), jnp.bfloat16),
            pltpu.VMEM((2, per_device, dates, dates), jnp.bfloat16),
            pltpu.VMEM((2, per_device, dates), jnp.float32),
            pltpu.VMEM((dates, LANES), jnp.float32),
            pltpu.VMEM((count, own_dates, LANES), jnp.float32),
            pltpu.SemaphoreType.DMA((groups, count)),
            pltpu.SemaphoreType.DMA((groups, count)),
            pltpu.SemaphoreType.DMA,
            pltpu.SemaphoreType.DMA((groups,)),
            pltpu.SemaphoreType.DMA((count,)),
            pltpu.SemaphoreType.DMA((count,)),
        ],
        compiler_params=pltpu.CompilerParams(collective_id=0, has_side_effects=True),
    )(blocks)


def solution(mesh):
    return jax.shard_map(
        local,
        mesh=mesh,
        in_specs=(
            P(None, None, "date", ("slab", "tile", "sub")),
            P(None, "date", ("slab", "tile", "sub")),
        ),
        out_specs=(
            P(None, ("slab", "tile", "sub"), "date", None, None, None),
            P(None, "date", ("slab", "tile", "sub")),
        ),
        check_vma=False,
    )
```

```python
import functools

import jax
import jax.numpy as jnp
from jax import lax
from jax.experimental import pallas as pl
from jax.experimental.pallas import tpu as pltpu
from jax.sharding import PartitionSpec as P

ITERS = 4
LANES = 128
NT = (((1,), (1,)), ((), ()))


def dot_nt(left, right):
    return lax.dot_general(left, right, NT, preferred_element_type=jnp.float32)


def window_coherence(real, imag, looks_count):
    dates = real.shape[0]
    plain = jnp.concatenate([real, imag], axis=1)
    swapped = jnp.concatenate([imag, -real], axis=1)
    sums = dot_nt(jnp.concatenate([plain, swapped], axis=0), plain)
    real_sum, imag_sum = sums[:dates], sums[dates:]
    rows = lax.broadcasted_iota(jnp.int32, (dates, dates), 0)
    columns = lax.broadcasted_iota(jnp.int32, (dates, dates), 1)
    diagonal = jnp.where(rows == columns, real_sum, 0.0)
    row_root = lax.rsqrt(jnp.sum(diagonal, axis=0, keepdims=True) * (1.0 / looks_count) + 1e-05)
    column_root = lax.rsqrt(jnp.sum(diagonal, axis=1, keepdims=True) * (1.0 / looks_count) + 1e-05)
    factor = column_root * row_root * (1.0 / looks_count)
    return (real_sum * factor).astype(jnp.bfloat16), (imag_sum * factor).astype(jnp.bfloat16)


def link_windows(matrices):
    dates = matrices[0].shape[1]
    row = lax.broadcasted_iota(jnp.int32, (8, dates), 0)
    is_real = row < 3
    is_imag = jnp.logical_and(row >= 3, row < 6)
    is_first = jnp.logical_or(row == 0, row == 3)
    is_second = jnp.logical_or(row == 1, row == 4)
    state = [jnp.where(is_real, 1.0, 0.0)] * len(matrices)
    result = None
    for step in range(ITERS):
        products = []
        for vec, matrix in zip(state, matrices):
            high = vec.astype(jnp.bfloat16).astype(jnp.float32)
            rest = vec - high
            middle = rest.astype(jnp.bfloat16).astype(jnp.float32)
            parts = jnp.where(is_first, high, jnp.where(is_second, middle, rest - middle))
            products.append(dot_nt(parts.astype(jnp.bfloat16), matrix))
        state, result = [], []
        for product in products:
            first, second = product[:, :dates], product[:, dates:]
            zero = jnp.zeros_like(first)
            new_real = jnp.sum(
                jnp.where(is_real, first, jnp.where(is_imag, -second, zero)), axis=0, keepdims=True
            )
            new_imag = jnp.sum(
                jnp.where(is_real, second, jnp.where(is_imag, first, zero)), axis=0, keepdims=True
            )
            power = jnp.sum(new_real * new_real + new_imag * new_imag, axis=1, keepdims=True)
            scale = lax.rsqrt(power * (1.0 / dates) + 1e-05)
            new_real = new_real * scale
            new_imag = new_imag * scale
            result.append((new_real, new_imag))
            state.append(
                jnp.where(
                    is_real,
                    jnp.broadcast_to(new_real, (8, dates)),
                    jnp.where(is_imag, jnp.broadcast_to(new_imag, (8, dates)), 0.0),
                )
            )
    return result


def send_order(count):
    middle = count // 2
    return sorted(range(1, count), key=lambda offset: abs(offset - middle))


def kernel(
    count, looks_count, group,
    block_ref, coherence_ref, linked_ref,
    packed, arrived, held, matrix, vectors, turned, landed,
    send_sem, recv_sem, out_sem, back_send, back_recv,
):
    me = lax.axis_index("date")
    windows = held.shape[0]
    dates = held.shape[2]
    own = dates // count
    groups = windows // group

    barrier = pltpu.get_barrier_semaphore()
    for offset in range(1, count):
        pl.semaphore_signal(
            barrier, inc=1, device_id={"date": lax.rem(me + offset, count)},
            device_id_type=pl.DeviceIdType.MESH,
        )

    mine = pl.ds(pl.multiple_of(me * own, own), own)
    order = send_order(count)

    def block_copy(part, offset):
        other = lax.rem(me + offset, count)
        return pltpu.make_async_remote_copy(
            src_ref=packed.at[other, part],
            dst_ref=arrived.at[part, me],
            send_sem=send_sem.at[part, offset],
            recv_sem=recv_sem.at[part, offset],
            device_id={"date": other},
            device_id_type=pl.DeviceIdType.MESH,
        )

    def pack(part, offset):
        other = lax.rem(me + offset, count)
        for side in range(2):
            packed[other, part, side] = block_ref[other, part, side].T

    pack(0, order[0])
    pl.semaphore_wait(barrier, count - 1)

    for part in range(groups):
        for place, offset in enumerate(order):
            if place + 1 < len(order):
                pack(part, order[place + 1])
            elif part + 1 < groups:
                pack(part + 1, order[0])
            block_copy(part, offset).start()

    held[:, :, :, looks_count:] = jnp.zeros(held.shape[:3] + (held.shape[3] - looks_count,), held.dtype)

    def out_copy(part):
        span = pl.ds(part * group, group)
        return pltpu.make_async_copy(
            matrix.at[:, span], coherence_ref.at[:, 0, 0, span], out_sem.at[part]
        )

    def place_rows(part, side, source, rows):
        span = pl.ds(pl.multiple_of(source * own, own), own)
        for inner in range(group):
            held[part * group + inner, side, span, :looks_count] = rows[inner * own : (inner + 1) * own]

    def compute_part(part, carry):
        for side in range(2):
            place_rows(part, side, me, block_ref[me, part, side])
        for offset in order:
            block_copy(part, offset).wait_recv()
            source = lax.rem(me + count - offset, count)
            for side in range(2):
                place_rows(part, side, source, arrived[part, source, side].T)
        matrices = []
        for inner in range(group):
            window = part * group + inner
            real, imag = window_coherence(held[window, 0], held[window, 1], looks_count)
            matrix[0, window] = real
            matrix[1, window] = imag
            matrices.append(jnp.concatenate([real, imag], axis=0))
        out_copy(part).start()
        for inner, (real, imag) in enumerate(link_windows(matrices)):
            vectors[0, pl.ds(part * group + inner, 1)] = real
            vectors[1, pl.ds(part * group + inner, 1)] = imag
        return carry

    lax.fori_loop(0, groups, compute_part, 0)

    turned[:, : 2 * windows] = jnp.concatenate([vectors[0], vectors[1]], axis=0).T

    def back_copy(offset):
        other = lax.rem(me + offset, count)
        return pltpu.make_async_remote_copy(
            src_ref=turned.at[pl.ds(pl.multiple_of(other * own, own), own)],
            dst_ref=landed.at[me],
            send_sem=back_send.at[offset],
            recv_sem=back_recv.at[offset],
            device_id={"date": other},
            device_id_type=pl.DeviceIdType.MESH,
        )

    for offset in range(1, count):
        back_copy(offset).start()
    landed[me] = turned[mine]
    for offset in range(1, count):
        back_copy(offset).wait_recv()
    for side in range(2):
        linked_ref[side] = jnp.concatenate(
            [landed[source][:, side * windows : (side + 1) * windows] for source in range(count)], axis=1
        )

    def finish_part(part, carry):
        for offset in range(1, count):
            block_copy(part, offset).wait_send()
        out_copy(part).wait()
        return carry

    lax.fori_loop(0, groups, finish_part, 0)
    for offset in range(1, count):
        back_copy(offset).wait_send()


def local(slc, usable):
    looks_count, own_dates, windows = usable.shape
    count = lax.axis_size("date")
    per_device = windows // count
    dates = own_dates * count
    masked = slc * usable.astype(jnp.bfloat16)[None]
    padded_looks = pl.cdiv(looks_count, LANES) * LANES
    group = min(per_device, max(1, LANES // own_dates))
    groups = per_device // group
    blocks = jnp.transpose(
        masked.reshape(2, looks_count, own_dates, count * groups, group), (3, 0, 4, 2, 1)
    ).reshape(count, groups, 2, group * own_dates, looks_count)
    return pl.pallas_call(
        functools.partial(kernel, count, looks_count, group),
        out_shape=(
            jax.ShapeDtypeStruct((2, 1, 1, per_device, dates, dates), jnp.bfloat16),
            jax.ShapeDtypeStruct((2, own_dates, windows), jnp.float32),
        ),
        in_specs=[pl.BlockSpec(memory_space=pltpu.VMEM)],
        out_specs=(
            pl.BlockSpec(memory_space=pl.ANY),
            pl.BlockSpec(memory_space=pltpu.VMEM),
        ),
        scratch_shapes=[
            pltpu.VMEM((count, groups, 2, looks_count, group * own_dates), jnp.bfloat16),
            pltpu.VMEM((groups, count, 2, looks_count, group * own_dates), jnp.bfloat16),
            pltpu.VMEM((per_device, 2, dates, padded_looks), jnp.bfloat16),
            pltpu.VMEM((2, per_device, dates, dates), jnp.bfloat16),
            pltpu.VMEM((2, per_device, dates), jnp.float32),
            pltpu.VMEM((dates, LANES), jnp.float32),
            pltpu.VMEM((count, own_dates, LANES), jnp.float32),
            pltpu.SemaphoreType.DMA((groups, count)),
            pltpu.SemaphoreType.DMA((groups, count)),
            pltpu.SemaphoreType.DMA((groups,)),
            pltpu.SemaphoreType.DMA((count,)),
            pltpu.SemaphoreType.DMA((count,)),
        ],
        compiler_params=pltpu.CompilerParams(collective_id=0, has_side_effects=True, vmem_limit_bytes=16 << 20),
    )(blocks)


def solution(mesh):
    return jax.shard_map(
        local,
        mesh=mesh,
        in_specs=(
            P(None, None, "date", ("slab", "tile", "sub")),
            P(None, "date", ("slab", "tile", "sub")),
        ),
        out_specs=(
            P(None, ("slab", "tile", "sub"), "date", None, None, None),
            P(None, "date", ("slab", "tile", "sub")),
        ),
        check_vma=False,
    )
```

```python
import functools

import jax
import jax.numpy as jnp
from jax import lax
from jax.experimental import pallas as pl
from jax.experimental.pallas import tpu as pltpu
from jax.sharding import PartitionSpec as P

ITERS = 4
LANES = 128
NT = (((1,), (1,)), ((), ()))


def dot_nt(left, right):
    return lax.dot_general(left, right, NT, preferred_element_type=jnp.float32)


def window_coherence(real, imag, looks_count):
    dates = real.shape[0]
    plain = jnp.concatenate([real, imag], axis=1)
    swapped = jnp.concatenate([imag, -real], axis=1)
    sums = dot_nt(jnp.concatenate([plain, swapped], axis=0), plain)
    real_sum, imag_sum = sums[:dates], sums[dates:]
    rows = lax.broadcasted_iota(jnp.int32, (dates, dates), 0)
    columns = lax.broadcasted_iota(jnp.int32, (dates, dates), 1)
    diagonal = jnp.where(rows == columns, real_sum, 0.0)
    row_root = lax.rsqrt(jnp.sum(diagonal, axis=0, keepdims=True) * (1.0 / looks_count) + 1e-05)
    column_root = lax.rsqrt(jnp.sum(diagonal, axis=1, keepdims=True) * (1.0 / looks_count) + 1e-05)
    factor = column_root * row_root * (1.0 / looks_count)
    return (real_sum * factor).astype(jnp.bfloat16), (imag_sum * factor).astype(jnp.bfloat16)


def link_windows(matrices):
    dates = matrices[0].shape[1]
    row = lax.broadcasted_iota(jnp.int32, (8, dates), 0)
    is_real = row < 3
    is_imag = jnp.logical_and(row >= 3, row < 6)
    is_first = jnp.logical_or(row == 0, row == 3)
    is_second = jnp.logical_or(row == 1, row == 4)
    state = [jnp.where(is_real, 1.0, 0.0)] * len(matrices)
    result = None
    for step in range(ITERS):
        products = []
        for vec, matrix in zip(state, matrices):
            high = vec.astype(jnp.bfloat16).astype(jnp.float32)
            rest = vec - high
            middle = rest.astype(jnp.bfloat16).astype(jnp.float32)
            parts = jnp.where(is_first, high, jnp.where(is_second, middle, rest - middle))
            products.append(dot_nt(parts.astype(jnp.bfloat16), matrix))
        state, result = [], []
        for product in products:
            first, second = product[:, :dates], product[:, dates:]
            zero = jnp.zeros_like(first)
            new_real = jnp.sum(
                jnp.where(is_real, first, jnp.where(is_imag, -second, zero)), axis=0, keepdims=True
            )
            new_imag = jnp.sum(
                jnp.where(is_real, second, jnp.where(is_imag, first, zero)), axis=0, keepdims=True
            )
            power = jnp.sum(new_real * new_real + new_imag * new_imag, axis=1, keepdims=True)
            scale = lax.rsqrt(power * (1.0 / dates) + 1e-05)
            new_real = new_real * scale
            new_imag = new_imag * scale
            result.append((new_real, new_imag))
            state.append(
                jnp.where(
                    is_real,
                    jnp.broadcast_to(new_real, (8, dates)),
                    jnp.where(is_imag, jnp.broadcast_to(new_imag, (8, dates)), 0.0),
                )
            )
    return result


def send_order(count):
    middle = count // 2
    return sorted(range(1, count), key=lambda offset: abs(offset - middle))


def kernel(
    count, looks_count, group,
    block_ref, coherence_ref, linked_ref,
    packed, arrived, held, matrix, vectors, turned, landed,
    send_sem, recv_sem, out_sem, back_send, back_recv,
):
    me = lax.axis_index("date")
    windows = held.shape[0]
    dates = held.shape[2]
    own = dates // count
    groups = windows // group

    barrier = pltpu.get_barrier_semaphore()
    for offset in range(1, count):
        pl.semaphore_signal(
            barrier, inc=1, device_id={"date": lax.rem(me + offset, count)},
            device_id_type=pl.DeviceIdType.MESH,
        )

    mine = pl.ds(pl.multiple_of(me * own, own), own)
    order = send_order(count)

    def block_copy(part, offset):
        other = lax.rem(me + offset, count)
        return pltpu.make_async_remote_copy(
            src_ref=packed.at[other, part],
            dst_ref=arrived.at[part, me],
            send_sem=send_sem.at[part, offset],
            recv_sem=recv_sem.at[part, offset],
            device_id={"date": other},
            device_id_type=pl.DeviceIdType.MESH,
        )

    def pack(part, offset):
        other = lax.rem(me + offset, count)
        for side in range(2):
            packed[other, part, side] = block_ref[other, part, :, side].reshape(group * own, looks_count).T

    for offset in order:
        pack(0, offset)
    pl.semaphore_wait(barrier, count - 1)
    for offset in order:
        block_copy(0, offset).start()
    for part in range(1, groups):
        for offset in order:
            pack(part, offset)
        for offset in order:
            block_copy(part, offset).start()

    held[:, :, :, looks_count:] = jnp.zeros(held.shape[:3] + (held.shape[3] - looks_count,), held.dtype)

    def out_copy(part):
        span = pl.ds(part * group, group)
        return pltpu.make_async_copy(
            matrix.at[:, span], coherence_ref.at[:, 0, 0, span], out_sem.at[part]
        )

    def place_rows(part, side, source, rows):
        span = pl.ds(pl.multiple_of(source * own, own), own)
        for inner in range(group):
            held[part * group + inner, side, span, :looks_count] = rows[inner * own : (inner + 1) * own]

    def compute_part(part, carry):
        for side in range(2):
            place_rows(part, side, me, block_ref[me, part, :, side].reshape(group * own, looks_count))
        for offset in order:
            block_copy(part, offset).wait_recv()
            source = lax.rem(me + count - offset, count)
            for side in range(2):
                place_rows(part, side, source, arrived[part, source, side].T)
        matrices = []
        for inner in range(group):
            window = part * group + inner
            real, imag = window_coherence(held[window, 0], held[window, 1], looks_count)
            matrix[0, window] = real
            matrix[1, window] = imag
            matrices.append(jnp.concatenate([real, imag], axis=0))
        out_copy(part).start()
        for inner, (real, imag) in enumerate(link_windows(matrices)):
            vectors[0, pl.ds(part * group + inner, 1)] = real
            vectors[1, pl.ds(part * group + inner, 1)] = imag
        return carry

    lax.fori_loop(0, groups, compute_part, 0)

    turned[:, : 2 * windows] = jnp.concatenate([vectors[0], vectors[1]], axis=0).T

    def back_copy(offset):
        other = lax.rem(me + offset, count)
        return pltpu.make_async_remote_copy(
            src_ref=turned.at[pl.ds(pl.multiple_of(other * own, own), own)],
            dst_ref=landed.at[me],
            send_sem=back_send.at[offset],
            recv_sem=back_recv.at[offset],
            device_id={"date": other},
            device_id_type=pl.DeviceIdType.MESH,
        )

    for offset in range(1, count):
        back_copy(offset).start()
    landed[me] = turned[mine]
    for offset in range(1, count):
        back_copy(offset).wait_recv()
    for side in range(2):
        linked_ref[side] = jnp.concatenate(
            [landed[source][:, side * windows : (side + 1) * windows] for source in range(count)], axis=1
        )

    def finish_part(part, carry):
        for offset in range(1, count):
            block_copy(part, offset).wait_send()
        out_copy(part).wait()
        return carry

    lax.fori_loop(0, groups, finish_part, 0)
    for offset in range(1, count):
        back_copy(offset).wait_send()


def local(slc, usable):
    looks_count, own_dates, windows = usable.shape
    count = lax.axis_size("date")
    per_device = windows // count
    dates = own_dates * count
    masked = slc * usable.astype(jnp.bfloat16)[None]
    padded_looks = pl.cdiv(looks_count, LANES) * LANES
    group = min(per_device, max(1, LANES // own_dates))
    groups = per_device // group
    blocks = jnp.transpose(
        masked.reshape(2, looks_count, own_dates, count, groups, group), (3, 4, 5, 0, 2, 1)
    )
    return pl.pallas_call(
        functools.partial(kernel, count, looks_count, group),
        out_shape=(
            jax.ShapeDtypeStruct((2, 1, 1, per_device, dates, dates), jnp.bfloat16),
            jax.ShapeDtypeStruct((2, own_dates, windows), jnp.float32),
        ),
        in_specs=[pl.BlockSpec(memory_space=pltpu.VMEM)],
        out_specs=(
            pl.BlockSpec(memory_space=pl.ANY),
            pl.BlockSpec(memory_space=pltpu.VMEM),
        ),
        scratch_shapes=[
            pltpu.VMEM((count, groups, 2, looks_count, group * own_dates), jnp.bfloat16),
            pltpu.VMEM((groups, count, 2, looks_count, group * own_dates), jnp.bfloat16),
            pltpu.VMEM((per_device, 2, dates, padded_looks), jnp.bfloat16),
            pltpu.VMEM((2, per_device, dates, dates), jnp.bfloat16),
            pltpu.VMEM((2, per_device, dates), jnp.float32),
            pltpu.VMEM((dates, LANES), jnp.float32),
            pltpu.VMEM((count, own_dates, LANES), jnp.float32),
            pltpu.SemaphoreType.DMA((groups, count)),
            pltpu.SemaphoreType.DMA((groups, count)),
            pltpu.SemaphoreType.DMA((groups,)),
            pltpu.SemaphoreType.DMA((count,)),
            pltpu.SemaphoreType.DMA((count,)),
        ],
        compiler_params=pltpu.CompilerParams(collective_id=0, has_side_effects=True, vmem_limit_bytes=16 << 20),
    )(blocks)


def solution(mesh):
    return jax.shard_map(
        local,
        mesh=mesh,
        in_specs=(
            P(None, None, "date", ("slab", "tile", "sub")),
            P(None, "date", ("slab", "tile", "sub")),
        ),
        out_specs=(
            P(None, ("slab", "tile", "sub"), "date", None, None, None),
            P(None, "date", ("slab", "tile", "sub")),
        ),
        check_vma=False,
    )
```

```python
import functools

import jax
import jax.numpy as jnp
from jax import lax
from jax.experimental import pallas as pl
from jax.experimental.pallas import tpu as pltpu
from jax.sharding import PartitionSpec as P

ITERS = 4
LANES = 128
NT = (((1,), (1,)), ((), ()))


def dot_nt(left, right):
    return lax.dot_general(left, right, NT, preferred_element_type=jnp.float32)


def window_coherence(real, imag, looks_count):
    dates = real.shape[0]
    plain = jnp.concatenate([real, imag], axis=1)
    swapped = jnp.concatenate([imag, -real], axis=1)
    sums = dot_nt(jnp.concatenate([plain, swapped], axis=0), plain)
    real_sum, imag_sum = sums[:dates], sums[dates:]
    rows = lax.broadcasted_iota(jnp.int32, (dates, dates), 0)
    columns = lax.broadcasted_iota(jnp.int32, (dates, dates), 1)
    diagonal = jnp.where(rows == columns, real_sum, 0.0)
    row_root = lax.rsqrt(jnp.sum(diagonal, axis=0, keepdims=True) * (1.0 / looks_count) + 1e-05)
    column_root = lax.rsqrt(jnp.sum(diagonal, axis=1, keepdims=True) * (1.0 / looks_count) + 1e-05)
    factor = column_root * row_root * (1.0 / looks_count)
    return (real_sum * factor).astype(jnp.bfloat16), (imag_sum * factor).astype(jnp.bfloat16)


def link_windows(matrices):
    dates = matrices[0].shape[1]
    row = lax.broadcasted_iota(jnp.int32, (8, dates), 0)
    is_real = row < 3
    is_imag = jnp.logical_and(row >= 3, row < 6)
    is_first = jnp.logical_or(row == 0, row == 3)
    is_second = jnp.logical_or(row == 1, row == 4)
    state = [jnp.where(is_real, 1.0, 0.0)] * len(matrices)
    result = None
    for step in range(ITERS):
        products = []
        for vec, matrix in zip(state, matrices):
            high = vec.astype(jnp.bfloat16).astype(jnp.float32)
            rest = vec - high
            middle = rest.astype(jnp.bfloat16).astype(jnp.float32)
            parts = jnp.where(is_first, high, jnp.where(is_second, middle, rest - middle))
            products.append(dot_nt(parts.astype(jnp.bfloat16), matrix))
        state, result = [], []
        for product in products:
            first, second = product[:, :dates], product[:, dates:]
            zero = jnp.zeros_like(first)
            new_real = jnp.sum(
                jnp.where(is_real, first, jnp.where(is_imag, -second, zero)), axis=0, keepdims=True
            )
            new_imag = jnp.sum(
                jnp.where(is_real, second, jnp.where(is_imag, first, zero)), axis=0, keepdims=True
            )
            power = jnp.sum(new_real * new_real + new_imag * new_imag, axis=1, keepdims=True)
            scale = lax.rsqrt(power * (1.0 / dates) + 1e-05)
            new_real = new_real * scale
            new_imag = new_imag * scale
            result.append((new_real, new_imag))
            state.append(
                jnp.where(
                    is_real,
                    jnp.broadcast_to(new_real, (8, dates)),
                    jnp.where(is_imag, jnp.broadcast_to(new_imag, (8, dates)), 0.0),
                )
            )
    return result


def send_order(count):
    middle = count // 2
    return sorted(range(1, count), key=lambda offset: (abs(offset - middle) > middle // 2, offset % 2 == 0, offset))


def kernel(
    count, looks_count, group,
    block_ref, coherence_ref, linked_ref,
    packed, arrived, held, matrix, vectors, turned, landed,
    send_sem, recv_sem, out_sem, back_send, back_recv,
):
    me = lax.axis_index("date")
    windows = held.shape[0]
    dates = held.shape[2]
    own = dates // count
    groups = windows // group

    barrier = pltpu.get_barrier_semaphore()
    for offset in range(1, count):
        pl.semaphore_signal(
            barrier, inc=1, device_id={"date": lax.rem(me + offset, count)},
            device_id_type=pl.DeviceIdType.MESH,
        )

    order = send_order(count)

    def block_copy(part, offset):
        other = lax.rem(me + offset, count)
        return pltpu.make_async_remote_copy(
            src_ref=packed.at[other, part],
            dst_ref=arrived.at[part, me],
            send_sem=send_sem.at[part, offset],
            recv_sem=recv_sem.at[part, offset],
            device_id={"date": other},
            device_id_type=pl.DeviceIdType.MESH,
        )

    def pack(part, offset):
        other = lax.rem(me + offset, count)
        packed[other, part] = jnp.concatenate(
            [block_ref[other, part, :, side].reshape(group * own, looks_count).T for side in range(2)], axis=0
        )

    for offset in order:
        pack(0, offset)
    pl.semaphore_wait(barrier, count - 1)
    for offset in order:
        block_copy(0, offset).start()
    for part in range(1, groups):
        for offset in order:
            pack(part, offset)
        for offset in order:
            block_copy(part, offset).start()

    held[:, :, :, looks_count:] = jnp.zeros(held.shape[:3] + (held.shape[3] - looks_count,), held.dtype)

    def out_copy(part):
        span = pl.ds(part * group, group)
        return pltpu.make_async_copy(
            matrix.at[:, span], coherence_ref.at[:, 0, 0, span], out_sem.at[part]
        )

    def place_rows(part, side, source, rows):
        span = pl.ds(pl.multiple_of(source * own, own), own)
        for inner in range(group):
            held[part * group + inner, side, span, :looks_count] = rows[inner * own : (inner + 1) * own]

    def compute_part(part, carry):
        for side in range(2):
            place_rows(part, side, me, block_ref[me, part, :, side].reshape(group * own, looks_count))
        for offset in order:
            block_copy(part, offset).wait_recv()
            source = lax.rem(me + count - offset, count)
            rows = arrived[part, source].T
            for side in range(2):
                place_rows(part, side, source, rows[:, side * looks_count : (side + 1) * looks_count])
        matrices = []
        for inner in range(group):
            window = part * group + inner
            real, imag = window_coherence(held[window, 0], held[window, 1], looks_count)
            matrix[0, window] = real
            matrix[1, window] = imag
            matrices.append(jnp.concatenate([real, imag], axis=0))
        out_copy(part).start()
        for inner, (real, imag) in enumerate(link_windows(matrices)):
            vectors[0, pl.ds(part * group + inner, 1)] = real
            vectors[1, pl.ds(part * group + inner, 1)] = imag
        return carry

    lax.fori_loop(0, groups, compute_part, 0)

    fold, rows, width = own // turned.shape[1], turned.shape[1], 2 * windows
    spread = jnp.concatenate([vectors[0], vectors[1]], axis=0)
    spread = jnp.pad(spread, ((0, LANES - width), (0, 0))).T.reshape(count, fold, rows, LANES)
    folded = spread[:, 0]
    for place in range(1, fold):
        folded = folded + pltpu.roll(
            spread[:, place].reshape(count * rows, LANES), place * width, 1
        ).reshape(count, rows, LANES)
    turned[...] = folded

    def back_copy(offset):
        other = lax.rem(me + offset, count)
        return pltpu.make_async_remote_copy(
            src_ref=turned.at[other],
            dst_ref=landed.at[me],
            send_sem=back_send.at[offset],
            recv_sem=back_recv.at[offset],
            device_id={"date": other},
            device_id_type=pl.DeviceIdType.MESH,
        )

    for offset in range(1, count):
        back_copy(offset).start()
    landed[me] = turned[me]
    for offset in range(1, count):
        back_copy(offset).wait_recv()
    for side in range(2):
        for place in range(fold):
            first = place * width + side * windows
            linked_ref[side, place * rows : (place + 1) * rows] = jnp.concatenate(
                [landed[source][:, first : first + windows] for source in range(count)], axis=1
            )

    def finish_part(part, carry):
        for offset in range(1, count):
            block_copy(part, offset).wait_send()
        out_copy(part).wait()
        return carry

    lax.fori_loop(0, groups, finish_part, 0)
    for offset in range(1, count):
        back_copy(offset).wait_send()


def local(slc, usable):
    looks_count, own_dates, windows = usable.shape
    count = lax.axis_size("date")
    per_device = windows // count
    dates = own_dates * count
    masked = slc * usable.astype(jnp.bfloat16)[None]
    padded_looks = pl.cdiv(looks_count, LANES) * LANES
    group = min(per_device, max(1, LANES // own_dates))
    groups = per_device // group
    fold = max(1, own_dates // 8)
    fold = fold if own_dates % fold == 0 and 2 * per_device * fold <= LANES else 1
    blocks = jnp.transpose(
        masked.reshape(2, looks_count, own_dates, count, groups, group), (3, 4, 5, 0, 2, 1)
    )
    return pl.pallas_call(
        functools.partial(kernel, count, looks_count, group),
        out_shape=(
            jax.ShapeDtypeStruct((2, 1, 1, per_device, dates, dates), jnp.bfloat16),
            jax.ShapeDtypeStruct((2, own_dates, windows), jnp.float32),
        ),
        in_specs=[pl.BlockSpec(memory_space=pltpu.VMEM)],
        out_specs=(
            pl.BlockSpec(memory_space=pl.ANY),
            pl.BlockSpec(memory_space=pltpu.VMEM),
        ),
        scratch_shapes=[
            pltpu.VMEM((count, groups, 2 * looks_count, group * own_dates), jnp.bfloat16),
            pltpu.VMEM((groups, count, 2 * looks_count, group * own_dates), jnp.bfloat16),
            pltpu.VMEM((per_device, 2, dates, padded_looks), jnp.bfloat16),
            pltpu.VMEM((2, per_device, dates, dates), jnp.bfloat16),
            pltpu.VMEM((2, per_device, dates), jnp.float32),
            pltpu.VMEM((count, own_dates // fold, LANES), jnp.float32),
            pltpu.VMEM((count, own_dates // fold, LANES), jnp.float32),
            pltpu.SemaphoreType.DMA((groups, count)),
            pltpu.SemaphoreType.DMA((groups, count)),
            pltpu.SemaphoreType.DMA((groups,)),
            pltpu.SemaphoreType.DMA((count,)),
            pltpu.SemaphoreType.DMA((count,)),
        ],
        compiler_params=pltpu.CompilerParams(collective_id=0, has_side_effects=True, vmem_limit_bytes=16 << 20),
    )(blocks)


def solution(mesh):
    return jax.shard_map(
        local,
        mesh=mesh,
        in_specs=(
            P(None, None, "date", ("slab", "tile", "sub")),
            P(None, "date", ("slab", "tile", "sub")),
        ),
        out_specs=(
            P(None, ("slab", "tile", "sub"), "date", None, None, None),
            P(None, "date", ("slab", "tile", "sub")),
        ),
        check_vma=False,
    )
```

```python
import functools

import jax
import jax.numpy as jnp
from jax import lax
from jax.experimental import pallas as pl
from jax.experimental.pallas import tpu as pltpu
from jax.sharding import PartitionSpec as P

ITERS = 4
LANES = 128
PIECES = 2
NT = (((1,), (1,)), ((), ()))


def dot_nt(left, right):
    return lax.dot_general(left, right, NT, preferred_element_type=jnp.float32)


def window_coherence(real, imag, looks_count):
    dates = real.shape[0]
    plain = jnp.concatenate([real, imag], axis=1)
    swapped = jnp.concatenate([imag, -real], axis=1)
    sums = dot_nt(jnp.concatenate([plain, swapped], axis=0), plain)
    real_sum, imag_sum = sums[:dates], sums[dates:]
    rows = lax.broadcasted_iota(jnp.int32, (dates, dates), 0)
    columns = lax.broadcasted_iota(jnp.int32, (dates, dates), 1)
    diagonal = jnp.where(rows == columns, real_sum, 0.0)
    row_root = lax.rsqrt(jnp.sum(diagonal, axis=0, keepdims=True) * (1.0 / looks_count) + 1e-05)
    column_root = lax.rsqrt(jnp.sum(diagonal, axis=1, keepdims=True) * (1.0 / looks_count) + 1e-05)
    factor = column_root * row_root * (1.0 / looks_count)
    return (real_sum * factor).astype(jnp.bfloat16), (imag_sum * factor).astype(jnp.bfloat16)


def link_windows(matrices):
    dates = matrices[0].shape[1]
    row = lax.broadcasted_iota(jnp.int32, (8, dates), 0)
    is_real = row < 3
    is_imag = jnp.logical_and(row >= 3, row < 6)
    is_first = jnp.logical_or(row == 0, row == 3)
    is_second = jnp.logical_or(row == 1, row == 4)
    state = [jnp.where(is_real, 1.0, 0.0)] * len(matrices)
    result = None
    for step in range(ITERS):
        products = []
        for vec, matrix in zip(state, matrices):
            high = vec.astype(jnp.bfloat16).astype(jnp.float32)
            rest = vec - high
            middle = rest.astype(jnp.bfloat16).astype(jnp.float32)
            parts = jnp.where(is_first, high, jnp.where(is_second, middle, rest - middle))
            products.append(dot_nt(parts.astype(jnp.bfloat16), matrix))
        state, result = [], []
        for product in products:
            first, second = product[:, :dates], product[:, dates:]
            zero = jnp.zeros_like(first)
            new_real = jnp.sum(
                jnp.where(is_real, first, jnp.where(is_imag, -second, zero)), axis=0, keepdims=True
            )
            new_imag = jnp.sum(
                jnp.where(is_real, second, jnp.where(is_imag, first, zero)), axis=0, keepdims=True
            )
            power = jnp.sum(new_real * new_real + new_imag * new_imag, axis=1, keepdims=True)
            scale = lax.rsqrt(power * (1.0 / dates) + 1e-05)
            new_real = new_real * scale
            new_imag = new_imag * scale
            result.append((new_real, new_imag))
            state.append(
                jnp.where(
                    is_real,
                    jnp.broadcast_to(new_real, (8, dates)),
                    jnp.where(is_imag, jnp.broadcast_to(new_imag, (8, dates)), 0.0),
                )
            )
    return result


def send_order(count):
    middle = count // 2
    return sorted(range(1, count), key=lambda offset: (abs(offset - middle) > middle // 2, offset % 2 == 0, offset))


def kernel(
    count, looks_count, group,
    block_ref, coherence_ref, linked_ref,
    packed, arrived, held, vectors, turned, landed,
    send_sem, recv_sem, back_send, back_recv,
):
    me = lax.axis_index("date")
    windows = held.shape[0]
    dates = held.shape[2]
    own = dates // count
    groups = windows // group

    barrier = pltpu.get_barrier_semaphore()
    for offset in range(1, count):
        pl.semaphore_signal(
            barrier, inc=1, device_id={"date": lax.rem(me + offset, count)},
            device_id_type=pl.DeviceIdType.MESH,
        )

    order = send_order(count)

    def block_copy(part, offset):
        other = lax.rem(me + offset, count)
        return pltpu.make_async_remote_copy(
            src_ref=packed.at[other, part],
            dst_ref=arrived.at[part, me],
            send_sem=send_sem.at[part, offset],
            recv_sem=recv_sem.at[part, offset],
            device_id={"date": other},
            device_id_type=pl.DeviceIdType.MESH,
        )

    def pack(part, offset):
        other = lax.rem(me + offset, count)
        packed[other, part] = jnp.concatenate(
            [block_ref[other, part, :, side].reshape(group * own, looks_count).T for side in range(2)], axis=0
        )

    for offset in order:
        pack(0, offset)
    pl.semaphore_wait(barrier, count - 1)
    for offset in order:
        block_copy(0, offset).start()
    for part in range(1, groups):
        for offset in order:
            pack(part, offset)
        for offset in order:
            block_copy(part, offset).start()

    held[:, :, :, looks_count:] = jnp.zeros(held.shape[:3] + (held.shape[3] - looks_count,), held.dtype)

    def place_rows(part, side, source, rows):
        span = pl.ds(pl.multiple_of(source * own, own), own)
        for inner in range(group):
            held[part * group + inner, side, span, :looks_count] = rows[inner * own : (inner + 1) * own]

    def compute_part(part, carry):
        for side in range(2):
            place_rows(part, side, me, block_ref[me, part, :, side].reshape(group * own, looks_count))
        for offset in order:
            block_copy(part, offset).wait_recv()
            source = lax.rem(me + count - offset, count)
            rows = arrived[part, source].T
            for side in range(2):
                place_rows(part, side, source, rows[:, side * looks_count : (side + 1) * looks_count])
        matrices = []
        for inner in range(group):
            window = part * group + inner
            real, imag = window_coherence(held[window, 0], held[window, 1], looks_count)
            coherence_ref[0, 0, 0, window] = real
            coherence_ref[1, 0, 0, window] = imag
            matrices.append(jnp.concatenate([real, imag], axis=0))
        for inner, (real, imag) in enumerate(link_windows(matrices)):
            vectors[0, pl.ds(part * group + inner, 1)] = real
            vectors[1, pl.ds(part * group + inner, 1)] = imag
        return carry

    lax.fori_loop(0, groups, compute_part, 0)

    fold, rows, width = own // turned.shape[1], turned.shape[1], 2 * windows
    spread = jnp.concatenate([vectors[0], vectors[1]], axis=0)
    spread = jnp.pad(spread, ((0, LANES - width), (0, 0))).T.reshape(count, fold, rows, LANES)
    folded = spread[:, 0]
    for place in range(1, fold):
        folded = folded + pltpu.roll(
            spread[:, place].reshape(count * rows, LANES), place * width, 1
        ).reshape(count, rows, LANES)
    turned[...] = folded

    def back_copy(offset):
        other = lax.rem(me + offset, count)
        return pltpu.make_async_remote_copy(
            src_ref=turned.at[other],
            dst_ref=landed.at[me],
            send_sem=back_send.at[offset],
            recv_sem=back_recv.at[offset],
            device_id={"date": other},
            device_id_type=pl.DeviceIdType.MESH,
        )

    for offset in range(1, count):
        back_copy(offset).start()
    landed[me] = turned[me]
    for offset in range(1, count):
        back_copy(offset).wait_recv()
    for side in range(2):
        for place in range(fold):
            first = place * width + side * windows
            linked_ref[side, place * rows : (place + 1) * rows] = jnp.concatenate(
                [landed[source][:, first : first + windows] for source in range(count)], axis=1
            )

    def finish_part(part, carry):
        for offset in range(1, count):
            block_copy(part, offset).wait_send()
        return carry

    lax.fori_loop(0, groups, finish_part, 0)
    for offset in range(1, count):
        back_copy(offset).wait_send()


def deliver(coherence_in, linked_in, coherence_out, linked_out, sem):
    copies = [pltpu.make_async_copy(linked_in, linked_out, sem.at[0])]
    windows = coherence_in.shape[3]
    pieces = PIECES if windows % PIECES == 0 else 1
    size = windows // pieces
    for side in range(coherence_in.shape[0]):
        for piece in range(pieces):
            span = pl.ds(piece * size, size)
            copies.append(
                pltpu.make_async_copy(
                    coherence_in.at[side, :, :, span],
                    coherence_out.at[side, :, :, span],
                    sem.at[1 + side * PIECES + piece],
                )
            )
    for copy in copies:
        copy.start()
    for copy in copies:
        copy.wait()


def local(slc, usable):
    looks_count, own_dates, windows = usable.shape
    count = lax.axis_size("date")
    per_device = windows // count
    dates = own_dates * count
    masked = slc * usable.astype(jnp.bfloat16)[None]
    padded_looks = pl.cdiv(looks_count, LANES) * LANES
    group = min(per_device, max(1, LANES // own_dates))
    groups = per_device // group
    fold = max(1, own_dates // 8)
    fold = fold if own_dates % fold == 0 and 2 * per_device * fold <= LANES else 1
    blocks = jnp.transpose(
        masked.reshape(2, looks_count, own_dates, count, groups, group), (3, 4, 5, 0, 2, 1)
    )
    results = pl.pallas_call(
        functools.partial(kernel, count, looks_count, group),
        out_shape=(
            jax.ShapeDtypeStruct((2, 1, 1, per_device, dates, dates), jnp.bfloat16),
            jax.ShapeDtypeStruct((2, own_dates, windows), jnp.float32),
        ),
        in_specs=[pl.BlockSpec(memory_space=pltpu.VMEM)],
        out_specs=(
            pl.BlockSpec(memory_space=pltpu.VMEM),
            pl.BlockSpec(memory_space=pltpu.VMEM),
        ),
        scratch_shapes=[
            pltpu.VMEM((count, groups, 2 * looks_count, group * own_dates), jnp.bfloat16),
            pltpu.VMEM((groups, count, 2 * looks_count, group * own_dates), jnp.bfloat16),
            pltpu.VMEM((per_device, 2, dates, padded_looks), jnp.bfloat16),
            pltpu.VMEM((2, per_device, dates), jnp.float32),
            pltpu.VMEM((count, own_dates // fold, LANES), jnp.float32),
            pltpu.VMEM((count, own_dates // fold, LANES), jnp.float32),
            pltpu.SemaphoreType.DMA((groups, count)),
            pltpu.SemaphoreType.DMA((groups, count)),
            pltpu.SemaphoreType.DMA((count,)),
            pltpu.SemaphoreType.DMA((count,)),
        ],
        compiler_params=pltpu.CompilerParams(collective_id=0, has_side_effects=True, vmem_limit_bytes=16 << 20),
    )(blocks)
    return pl.pallas_call(
        deliver,
        out_shape=tuple(jax.ShapeDtypeStruct(array.shape, array.dtype) for array in results),
        in_specs=[pl.BlockSpec(memory_space=pl.ANY)] * 2,
        out_specs=(pl.BlockSpec(memory_space=pl.ANY),) * 2,
        scratch_shapes=[pltpu.SemaphoreType.DMA((results[0].shape[0] * PIECES + 1,))],
        compiler_params=pltpu.CompilerParams(vmem_limit_bytes=1 << 20),
    )(*results)


def solution(mesh):
    return jax.shard_map(
        local,
        mesh=mesh,
        in_specs=(
            P(None, None, "date", ("slab", "tile", "sub")),
            P(None, "date", ("slab", "tile", "sub")),
        ),
        out_specs=(
            P(None, ("slab", "tile", "sub"), "date", None, None, None),
            P(None, "date", ("slab", "tile", "sub")),
        ),
        check_vma=False,
    )
```

```python
import functools

import jax
import jax.numpy as jnp
from jax import lax
from jax.experimental import pallas as pl
from jax.experimental.pallas import tpu as pltpu
from jax.sharding import PartitionSpec as P

ITERS = 4
LANES = 128
PIECES = 2
NT = (((1,), (1,)), ((), ()))


def dot_nt(left, right):
    return lax.dot_general(left, right, NT, preferred_element_type=jnp.float32)


def window_coherence(real, imag, looks_count):
    dates = real.shape[0]
    plain = jnp.concatenate([real, imag], axis=1)
    swapped = jnp.concatenate([imag, -real], axis=1)
    sums = dot_nt(jnp.concatenate([plain, swapped], axis=0), plain)
    real_sum, imag_sum = sums[:dates], sums[dates:]
    rows = lax.broadcasted_iota(jnp.int32, (dates, dates), 0)
    columns = lax.broadcasted_iota(jnp.int32, (dates, dates), 1)
    diagonal = jnp.where(rows == columns, real_sum, 0.0)
    row_root = lax.rsqrt(jnp.sum(diagonal, axis=0, keepdims=True) * (1.0 / looks_count) + 1e-05)
    column_root = lax.rsqrt(jnp.sum(diagonal, axis=1, keepdims=True) * (1.0 / looks_count) + 1e-05)
    factor = column_root * row_root * (1.0 / looks_count)
    return (real_sum * factor).astype(jnp.bfloat16), (imag_sum * factor).astype(jnp.bfloat16)


def link_windows(matrices):
    dates = matrices[0].shape[1]
    row = lax.broadcasted_iota(jnp.int32, (8, dates), 0)
    is_real = row < 3
    is_imag = jnp.logical_and(row >= 3, row < 6)
    is_first = jnp.logical_or(row == 0, row == 3)
    is_second = jnp.logical_or(row == 1, row == 4)
    state = [jnp.where(is_real, 1.0, 0.0)] * len(matrices)
    result = None
    for step in range(ITERS):
        products = []
        for vec, matrix in zip(state, matrices):
            high = vec.astype(jnp.bfloat16).astype(jnp.float32)
            rest = vec - high
            middle = rest.astype(jnp.bfloat16).astype(jnp.float32)
            parts = jnp.where(is_first, high, jnp.where(is_second, middle, rest - middle))
            products.append(dot_nt(parts.astype(jnp.bfloat16), matrix))
        state, result = [], []
        for product in products:
            first, second = product[:, :dates], product[:, dates:]
            zero = jnp.zeros_like(first)
            new_real = jnp.sum(
                jnp.where(is_real, first, jnp.where(is_imag, -second, zero)), axis=0, keepdims=True
            )
            new_imag = jnp.sum(
                jnp.where(is_real, second, jnp.where(is_imag, first, zero)), axis=0, keepdims=True
            )
            power = jnp.sum(new_real * new_real + new_imag * new_imag, axis=1, keepdims=True)
            scale = lax.rsqrt(power * (1.0 / dates) + 1e-05)
            new_real = new_real * scale
            new_imag = new_imag * scale
            result.append((new_real, new_imag))
            state.append(
                jnp.where(
                    is_real,
                    jnp.broadcast_to(new_real, (8, dates)),
                    jnp.where(is_imag, jnp.broadcast_to(new_imag, (8, dates)), 0.0),
                )
            )
    return result


def send_order(count):
    middle = count // 2
    return sorted(range(1, count), key=lambda offset: (offset % 2 == 0, -abs(offset - middle), offset))


def kernel(
    count, looks_count, group,
    block_ref, coherence_ref, linked_ref,
    packed, arrived, held, vectors, turned, landed,
    send_sem, recv_sem, back_send, back_recv,
):
    me = lax.axis_index("date")
    windows = held.shape[0]
    dates = held.shape[2]
    own = dates // count
    groups = windows // group

    barrier = pltpu.get_barrier_semaphore()
    for offset in range(1, count):
        pl.semaphore_signal(
            barrier, inc=1, device_id={"date": lax.rem(me + offset, count)},
            device_id_type=pl.DeviceIdType.MESH,
        )

    order = send_order(count)

    def block_copy(part, offset):
        other = lax.rem(me + offset, count)
        return pltpu.make_async_remote_copy(
            src_ref=packed.at[other, part],
            dst_ref=arrived.at[part, me],
            send_sem=send_sem.at[part, offset],
            recv_sem=recv_sem.at[part, offset],
            device_id={"date": other},
            device_id_type=pl.DeviceIdType.MESH,
        )

    def pack(part, offset):
        other = lax.rem(me + offset, count)
        packed[other, part] = jnp.concatenate(
            [block_ref[other, part, :, side].reshape(group * own, looks_count).T for side in range(2)], axis=0
        )

    for offset in order:
        pack(0, offset)
    pl.semaphore_wait(barrier, count - 1)
    for offset in order:
        block_copy(0, offset).start()
    for part in range(1, groups):
        for offset in order:
            pack(part, offset)
        for offset in order:
            block_copy(part, offset).start()

    held[:, :, :, looks_count:] = jnp.zeros(held.shape[:3] + (held.shape[3] - looks_count,), held.dtype)

    def place_rows(part, side, source, rows):
        span = pl.ds(pl.multiple_of(source * own, own), own)
        for inner in range(group):
            held[part * group + inner, side, span, :looks_count] = rows[inner * own : (inner + 1) * own]

    def compute_part(part, carry):
        for side in range(2):
            place_rows(part, side, me, block_ref[me, part, :, side].reshape(group * own, looks_count))
        for offset in order:
            block_copy(part, offset).wait_recv()
            source = lax.rem(me + count - offset, count)
            rows = arrived[part, source].T
            for side in range(2):
                place_rows(part, side, source, rows[:, side * looks_count : (side + 1) * looks_count])
        matrices = []
        for inner in range(group):
            window = part * group + inner
            real, imag = window_coherence(held[window, 0], held[window, 1], looks_count)
            coherence_ref[0, 0, 0, window] = real
            coherence_ref[1, 0, 0, window] = imag
            matrices.append(jnp.concatenate([real, imag], axis=0))
        for inner, (real, imag) in enumerate(link_windows(matrices)):
            vectors[0, pl.ds(part * group + inner, 1)] = real
            vectors[1, pl.ds(part * group + inner, 1)] = imag
        return carry

    lax.fori_loop(0, groups, compute_part, 0)

    fold, rows, width = own // turned.shape[1], turned.shape[1], 2 * windows
    spread = jnp.concatenate([vectors[0], vectors[1]], axis=0)
    spread = jnp.pad(spread, ((0, LANES - width), (0, 0))).T.reshape(count, fold, rows, LANES)
    folded = spread[:, 0]
    for place in range(1, fold):
        folded = folded + pltpu.roll(
            spread[:, place].reshape(count * rows, LANES), place * width, 1
        ).reshape(count, rows, LANES)
    turned[...] = folded

    def back_copy(offset):
        other = lax.rem(me + offset, count)
        return pltpu.make_async_remote_copy(
            src_ref=turned.at[other],
            dst_ref=landed.at[me],
            send_sem=back_send.at[offset],
            recv_sem=back_recv.at[offset],
            device_id={"date": other},
            device_id_type=pl.DeviceIdType.MESH,
        )

    for offset in range(1, count):
        back_copy(offset).start()
    landed[me] = turned[me]
    for offset in range(1, count):
        back_copy(offset).wait_recv()
    for side in range(2):
        for place in range(fold):
            first = place * width + side * windows
            linked_ref[side, place * rows : (place + 1) * rows] = jnp.concatenate(
                [landed[source][:, first : first + windows] for source in range(count)], axis=1
            )

    def finish_part(part, carry):
        for offset in range(1, count):
            block_copy(part, offset).wait_send()
        return carry

    lax.fori_loop(0, groups, finish_part, 0)
    for offset in range(1, count):
        back_copy(offset).wait_send()


def deliver(coherence_in, linked_in, coherence_out, linked_out, sem):
    copies = [pltpu.make_async_copy(linked_in, linked_out, sem.at[0])]
    windows = coherence_in.shape[3]
    pieces = PIECES if windows % PIECES == 0 else 1
    size = windows // pieces
    for side in range(coherence_in.shape[0]):
        for piece in range(pieces):
            span = pl.ds(piece * size, size)
            copies.append(
                pltpu.make_async_copy(
                    coherence_in.at[side, :, :, span],
                    coherence_out.at[side, :, :, span],
                    sem.at[1 + side * PIECES + piece],
                )
            )
    for copy in copies:
        copy.start()
    for copy in copies:
        copy.wait()


def local(slc, usable):
    looks_count, own_dates, windows = usable.shape
    count = lax.axis_size("date")
    per_device = windows // count
    dates = own_dates * count
    masked = slc * usable.astype(jnp.bfloat16)[None]
    padded_looks = pl.cdiv(looks_count, LANES) * LANES
    group = min(per_device, max(1, LANES // own_dates))
    groups = per_device // group
    fold = max(1, own_dates // 8)
    fold = fold if own_dates % fold == 0 and 2 * per_device * fold <= LANES else 1
    blocks = jnp.transpose(
        masked.reshape(2, looks_count, own_dates, count, groups, group), (3, 4, 5, 0, 2, 1)
    )
    results = pl.pallas_call(
        functools.partial(kernel, count, looks_count, group),
        out_shape=(
            jax.ShapeDtypeStruct((2, 1, 1, per_device, dates, dates), jnp.bfloat16),
            jax.ShapeDtypeStruct((2, own_dates, windows), jnp.float32),
        ),
        in_specs=[pl.BlockSpec(memory_space=pltpu.VMEM)],
        out_specs=(
            pl.BlockSpec(memory_space=pltpu.VMEM),
            pl.BlockSpec(memory_space=pltpu.VMEM),
        ),
        scratch_shapes=[
            pltpu.VMEM((count, groups, 2 * looks_count, group * own_dates), jnp.bfloat16),
            pltpu.VMEM((groups, count, 2 * looks_count, group * own_dates), jnp.bfloat16),
            pltpu.VMEM((per_device, 2, dates, padded_looks), jnp.bfloat16),
            pltpu.VMEM((2, per_device, dates), jnp.float32),
            pltpu.VMEM((count, own_dates // fold, LANES), jnp.float32),
            pltpu.VMEM((count, own_dates // fold, LANES), jnp.float32),
            pltpu.SemaphoreType.DMA((groups, count)),
            pltpu.SemaphoreType.DMA((groups, count)),
            pltpu.SemaphoreType.DMA((count,)),
            pltpu.SemaphoreType.DMA((count,)),
        ],
        compiler_params=pltpu.CompilerParams(collective_id=0, has_side_effects=True, vmem_limit_bytes=16 << 20),
    )(blocks)
    return pl.pallas_call(
        deliver,
        out_shape=tuple(jax.ShapeDtypeStruct(array.shape, array.dtype) for array in results),
        in_specs=[pl.BlockSpec(memory_space=pl.ANY)] * 2,
        out_specs=(pl.BlockSpec(memory_space=pl.ANY),) * 2,
        scratch_shapes=[pltpu.SemaphoreType.DMA((results[0].shape[0] * PIECES + 1,))],
        compiler_params=pltpu.CompilerParams(vmem_limit_bytes=1 << 20),
    )(*results)


def solution(mesh):
    return jax.shard_map(
        local,
        mesh=mesh,
        in_specs=(
            P(None, None, "date", ("slab", "tile", "sub")),
            P(None, "date", ("slab", "tile", "sub")),
        ),
        out_specs=(
            P(None, ("slab", "tile", "sub"), "date", None, None, None),
            P(None, "date", ("slab", "tile", "sub")),
        ),
        check_vma=False,
    )
```
